128 devices in a mesh: rep: 2 (over core), dp: 64 (over x, y, z).
Axes of the slice: x: 4, y: 4, z: 4, core: 2. Of those that a mesh axis runs over, the one named last changes fastest.
Arguments:
- x: bfloat16 [128, 1024, 512], P(('rep', 'dp')), parts along dimension 0
- dy: bfloat16 [128, 1024, 512], P(('rep', 'dp')), parts along dimension 0
- wq: bfloat16 [1, 512, 2048], replicated
- wk: bfloat16 [1, 512, 2048], replicated
- wv: bfloat16 [1, 512, 2048], replicated
- wo: bfloat16 [1, 2048, 512], replicated
- w_gate: bfloat16 [1, 512, 8192], replicated
- w_up: bfloat16 [1, 512, 8192], replicated
- w_down: bfloat16 [1, 8192, 512], replicated
- m_wq: float32 [1, 512, 2048], replicated
- m_wk: float32 [1, 512, 2048], replicated
- m_wv: float32 [1, 512, 2048], replicated
- m_wo: float32 [1, 2048, 512], replicated
- m_w_gate: float32 [1, 512, 8192], replicated
- m_w_up: float32 [1, 512, 8192], replicated
- m_w_down: float32 [1, 8192, 512], replicated
- v_wq: float32 [1, 512, 2048], replicated
- v_wk: float32 [1, 512, 2048], replicated
- v_wv: float32 [1, 512, 2048], replicated
- v_wo: float32 [1, 2048, 512], replicated
- v_w_gate: float32 [1, 512, 8192], replicated
- v_w_up: float32 [1, 512, 8192], replicated
- v_w_down: float32 [1, 8192, 512], replicated
Outputs:
- output 1: bfloat16 [2, 512, 2048], P('rep'), parts along dimension 0
- output 2: bfloat16 [2, 512, 2048], P('rep'), parts along dimension 0
- output 3: bfloat16 [2, 512, 2048], P('rep'), parts along dimension 0
- output 4: bfloat16 [2, 2048, 512], P('rep'), parts along dimension 0
- output 5: bfloat16 [2, 512, 8192], P('rep'), parts along dimension 0
- output 6: bfloat16 [2, 512, 8192], P('rep'), parts along dimension 0
- output 7: bfloat16 [2, 8192, 512], P('rep'), parts along dimension 0
- output 8: float32 [2, 512, 2048], P('rep'), parts along dimension 0
- output 9: float32 [2, 512, 2048], P('rep'), parts along dimension 0
- output 10: float32 [2, 512, 2048], P('rep'), parts along dimension 0
- output 11: float32 [2, 2048, 512], P('rep'), parts along dimension 0
- output 12: float32 [2, 512, 8192], P('rep'), parts along dimension 0
- output 13: float32 [2, 512, 8192], P('rep'), parts along dimension 0
- output 14: float32 [2, 8192, 512], P('rep'), parts along dimension 0
- output 15: float32 [2, 512, 2048], P('rep'), parts along dimension 0
- output 16: float32 [2, 512, 2048], P('rep'), parts along dimension 0
- output 17: float32 [2, 512, 2048], P('rep'), parts along dimension 0
- output 18: float32 [2, 2048, 512], P('rep'), parts along dimension 0
- output 19: float32 [2, 512, 8192], P('rep'), parts along dimension 0
- output 20: float32 [2, 512, 8192], P('rep'), parts along dimension 0
- output 21: float32 [2, 8192, 512], P('rep'), parts along dimension 0
There are 2 independent parts. The reference program is written for one: setup_inputs(seed, part) draws one part's arguments, and reference() takes and returns one part's arrays. A program takes and returns all parts, laid end to end along the dimension named above; an argument that names none is the same for every part.
All inputs are finite; a program needn't handle non-finite values.
Results may differ from the reference program's by a relative error of at most 0.024.
Values are sent between devices in bfloat16 or wider.
A program may use at most 1.5 GiB of HBM per device.

```python
import jax
import jax.numpy as jnp
from jax import lax

SEQUENCES = 64
TOKENS = 1024
D = 512
HEADS = 16
KV_HEADS = 16
HEAD = 128
FF = 8192
LAYERS = 1
THETA = 10000
NAMES = ("wq", "wk", "wv", "wo", "w_gate", "w_up", "w_down")
SHAPES = {
    "wq": (LAYERS, D, HEADS * HEAD),
    "wk": (LAYERS, D, KV_HEADS * HEAD),
    "wv": (LAYERS, D, KV_HEADS * HEAD),
    "wo": (LAYERS, HEADS * HEAD, D),
    "w_gate": (LAYERS, D, FF),
    "w_up": (LAYERS, D, FF),
    "w_down": (LAYERS, FF, D),
}


def bump(key, n, height):
    away = (jnp.arange(n, dtype=jnp.int32) - jax.random.randint(key, (), 0, n, jnp.int32)) % n
    return jnp.where(away < n // 8, height, 1.0)


def together(key, own, strength):
    shared = jax.random.normal(key, own.shape[1:], jnp.float32)
    return (own + strength * shared) * lax.rsqrt(1 + strength * strength)


def setup_inputs(seed: int = 0, part: int = 0) -> dict:
    kx, kdy, ka, kb, kz, kf, kh, kl, *keys = jax.random.split(jax.random.key(seed), 8 + 3 * len(NAMES))
    kx, kdy, ka, kb = (jax.random.fold_in(k, part) for k in (kx, kdy, ka, kb))
    kw, km, kv = (keys[i::3] for i in range(3))
    shape = (SEQUENCES, TOKENS, D)
    much_x, much_dy = jax.random.uniform(kz, (2,), jnp.float32, 0.0, 1.0)
    loud = 2.0 ** jax.random.uniform(jax.random.fold_in(kz, 1), (), jnp.float32, -1.0, 2.0)
    layers = 2.0 ** jax.random.uniform(kl, (LAYERS, 1, 1), jnp.float32, -1.0, 1.0)
    times = {"wq": 1.0, "wk": 1.0, "wv": 2.0, "wo": layers, "w_gate": 1.0, "w_up": bump(kh, FF, 4.0), "w_down": layers}
    x = together(ka, jax.random.normal(kx, shape, jnp.float32), much_x) * bump(kf, D, 4.0)
    dy = together(kb, jax.random.normal(kdy, shape, jnp.float32), much_dy)
    drawn = {"x": x.astype(jnp.bfloat16), "dy": (loud * dy * (SEQUENCES * TOKENS) ** -0.5).astype(jnp.bfloat16)}
    for key, name in zip(kw, NAMES, strict=True):
        drawn[name] = (jax.random.normal(key, SHAPES[name], jnp.float32) * SHAPES[name][1] ** -0.5 * times[name]).astype(jnp.bfloat16)
    for key, name in zip(km, NAMES, strict=True):
        drawn[f"m_{name}"] = 0.1 * jax.random.normal(key, SHAPES[name], jnp.float32)
    for key, name in zip(kv, NAMES, strict=True):
        drawn[f"v_{name}"] = loud * loud * jax.random.uniform(key, SHAPES[name], jnp.float32, 0.2, 0.6)
    return drawn


def matmul(a, w):
    return jnp.dot(a, w, preferred_element_type=jnp.float32).astype(jnp.bfloat16)


def normed(h):
    wide = h.astype(jnp.float32)
    scale = lax.rsqrt(jnp.mean(wide**2, -1, keepdims=True) + 1e-6)
    return (wide * scale).astype(jnp.bfloat16)


def turned(t, theta):
    half = t.shape[-1] // 2
    angle = jnp.arange(t.shape[0], dtype=jnp.float32)[:, None] * theta ** (-jnp.arange(half, dtype=jnp.float32) / half)
    cos, sin = jnp.cos(angle)[:, None], jnp.sin(angle)[:, None]
    a, b = t[..., :half].astype(jnp.float32), t[..., half:].astype(jnp.float32)
    return jnp.concatenate([a * cos - b * sin, b * cos + a * sin], -1).astype(jnp.bfloat16)


def seen_by(q, k, v):
    tokens, kv = q.shape[0], k.shape[1]
    q = q.reshape(tokens, kv, -1, q.shape[-1])
    scores = jnp.einsum("tgsd,ugd->gstu", q.astype(jnp.float32), k.astype(jnp.float32)) * q.shape[-1] ** -0.5
    place = jnp.arange(tokens)
    weights = jax.nn.softmax(jnp.where(place[:, None] >= place, scores, -jnp.inf), -1).astype(jnp.bfloat16)
    return jnp.einsum("gstu,ugd->tgsd", weights.astype(jnp.float32), v.astype(jnp.float32)).astype(jnp.bfloat16).reshape(tokens, -1)


def layer(h, w):
    a = normed(h)
    q, k = (turned(matmul(a, w[name]).reshape(h.shape[0], -1, HEAD), THETA) for name in ("wq", "wk"))
    h = h + matmul(seen_by(q, k, matmul(a, w["wv"]).reshape(h.shape[0], -1, HEAD)), w["wo"])
    b = normed(h)
    gate = jnp.dot(b, w["w_gate"], preferred_element_type=jnp.float32)
    up = jnp.dot(b, w["w_up"], preferred_element_type=jnp.float32)
    return h + matmul((jax.nn.silu(gate) * up).astype(jnp.bfloat16), w["w_down"])


def adamw(w, m, v, g):
    m = 0.9 * m + 0.1 * g
    v = 0.95 * v + 0.05 * g * g
    step = m * lax.rsqrt(v + 1e-8) + 0.1 * w
    return (w - 0.02 * step).astype(jnp.bfloat16), m, v


def stack(weights, h):
    return lax.scan(lambda h, w: (layer(h, w), None), h, weights)[0]


def reference(x, dy, wq, wk, wv, wo, w_gate, w_up, w_down, m_wq, m_wk, m_wv, m_wo, m_w_gate, m_w_up, m_w_down, v_wq, v_wk, v_wv, v_wo, v_w_gate, v_w_up, v_w_down):
    weights = dict(zip(NAMES, (wq, wk, wv, wo, w_gate, w_up, w_down), strict=True))

    def take(so_far, sequence):
        h, by_y = sequence
        _, back = jax.vjp(stack, weights, h)
        by_weights, by_h = back(by_y)
        return jax.tree.map(lambda total, term: total + term.astype(jnp.float32), so_far, by_weights), by_h

    none_yet = {name: jnp.zeros(w.shape, jnp.float32) for name, w in weights.items()}
    by_weights, by_x = lax.scan(take, none_yet, (x, dy))
    gradients = [by_weights[name].astype(jnp.bfloat16).astype(jnp.float32) for name in NAMES]
    first = (m_wq, m_wk, m_wv, m_wo, m_w_gate, m_w_up, m_w_down)
    second = (v_wq, v_wk, v_wv, v_wo, v_w_gate, v_w_up, v_w_down)
    new = [adamw(weights[name].astype(jnp.float32), m, v, g) for name, m, v, g in zip(NAMES, first, second, gradients, strict=True)]
    return tuple(one[which] for which in range(3) for one in new)
```

```python
import functools

import jax
import jax.numpy as jnp
from jax import lax
from jax.experimental import pallas as pl
from jax.experimental.pallas import tpu as pltpu
from jax.sharding import PartitionSpec as P

HEAD = 128
THETA = 10000
LOG2E = 1.4426950408889634
HIDDEN = -1e30
VMEM = 60 * 2**20
F32, BF16 = jnp.float32, jnp.bfloat16
QB = 256
PAIR = 256
FT = 512


def _nn(a, b):
    return lax.dot_general(a, b, (((1,), (0,)), ((), ())), preferred_element_type=F32)


def _nt(a, b):
    return lax.dot_general(a, b, (((1,), (1,)), ((), ())), preferred_element_type=F32)


def _tn(a, b):
    return lax.dot_general(a, b, (((0,), (0,)), ((), ())), preferred_element_type=F32)


def _normed(h):
    wide = h.astype(F32)
    scale = lax.rsqrt(jnp.mean(wide * wide, -1, keepdims=True) + 1e-6)
    return (wide * scale).astype(BF16)


def _attn_fwd(h_ref, cos_ref, sin_ref, wq_ref, wk_ref, wv_ref, wo_ref, q_ref, k_ref, v_ref, ot_ref, lse_ref, h1_ref, a_s, ot_s):
    step = pl.program_id(0)
    tokens = h_ref.shape[0]
    scale = HEAD**-0.5
    e = scale * LOG2E

    @pl.when(step == 0)
    def _():
        a_s[...] = _normed(h_ref[...])

    a = a_s[...]
    for w_ref, o_ref in ((wq_ref, q_ref), (wk_ref, k_ref)):
        t = _nn(a, w_ref[...]).astype(BF16).astype(F32)
        for j in range(PAIR // HEAD):
            one = t[:, j * HEAD : (j + 1) * HEAD]
            o_ref[:, j * HEAD : (j + 1) * HEAD] = (one * cos_ref[...] + pltpu.roll(one, HEAD // 2, 1) * sin_ref[...]).astype(BF16)
    v_ref[...] = _nn(a, wv_ref[...]).astype(BF16)

    seen = lax.broadcasted_iota(jnp.int32, (QB, QB), 0) <= lax.broadcasted_iota(jnp.int32, (QB, QB), 1)
    for j in range(PAIR // HEAD):
        cols = slice(j * HEAD, (j + 1) * HEAD)
        vt = v_ref[:, cols].T
        for i in range(tokens // QB):
            end = (i + 1) * QB
            q = q_ref[i * QB : end, cols]
            parts = []
            if i:
                parts.append(_nt(k_ref[: i * QB, cols], q))
            parts.append(jnp.where(seen, _nt(k_ref[i * QB : end, cols], q), HIDDEN))
            top = functools.reduce(jnp.maximum, [s.max(axis=0, keepdims=True) for s in parts])
            weights = [jnp.exp2((s - top) * e) for s in parts]
            total = sum(w.sum(axis=0, keepdims=True) for w in weights)
            p = jnp.concatenate([w.astype(BF16) for w in weights], axis=0)
            o = (_nn(vt[:, :end], p) * (1 / total)).astype(BF16)
            ot_ref[cols, i * QB : end] = o
            ot_s[pl.ds(step * PAIR + j * HEAD, HEAD), i * QB : end] = o
            lse_ref[pl.ds(step * 2 + j, 1), i * QB : end] = top * scale + jnp.log(total)

    @pl.when(step == pl.num_programs(0) - 1)
    def _():
        mixed = _tn(wo_ref[...], ot_s[...]).astype(BF16).T
        h1_ref[...] = h_ref[...] + mixed


def attn_fwd(h, cos, sin, wq, wk, wv, wo):
    tokens, d = h.shape
    width = wq.shape[1]
    whole = lambda s: (0, 0)
    cols = lambda s: (0, s)
    return pl.pallas_call(
        _attn_fwd,
        grid=(width // PAIR,),
        in_specs=[pl.BlockSpec((tokens, d), whole), pl.BlockSpec((tokens, HEAD), whole), pl.BlockSpec((tokens, HEAD), whole)]
        + [pl.BlockSpec((d, PAIR), cols)] * 3 + [pl.BlockSpec((width, d), whole)],
        out_specs=[pl.BlockSpec((tokens, PAIR), cols)] * 3 + [pl.BlockSpec((PAIR, tokens), lambda s: (s, 0)),
                   pl.BlockSpec((width // HEAD, tokens), whole), pl.BlockSpec((tokens, d), whole)],
        out_shape=[jax.ShapeDtypeStruct((tokens, width), BF16)] * 3 + [jax.ShapeDtypeStruct((width, tokens), BF16),
                   jax.ShapeDtypeStruct((width // HEAD, tokens), F32), jax.ShapeDtypeStruct((tokens, d), BF16)],
        scratch_shapes=[pltpu.VMEM((tokens, d), BF16), pltpu.VMEM((width, tokens), BF16)],
        compiler_params=pltpu.CompilerParams(dimension_semantics=("arbitrary",), vmem_limit_bytes=VMEM),
        cost_estimate=pl.CostEstimate(flops=20 * 10**9, transcendentals=10**7, bytes_accessed=40 * 10**6),
        name="attn_fwd",
    )(h, cos, sin, wq, wk, wv, wo)


ROW, LANE, TILES, SIDE, SLOTS = 16, 128, 128, 4, 3
CHUNKS = (32, 8, 2)
SUMS = 6


def _rem(a, n):
    return lax.rem(a, jnp.int32(n))


def _spots():
    d = lax.axis_index("dp")
    out = []
    for stride in (SIDE * SIDE, SIDE, 1):
        places = [_rem(lax.div(d, jnp.int32(stride)) + n, SIDE) for n in range(SIDE)]
        out.append((places, [d + (places[n] - places[0]) * stride for n in (1, -1)]))
    return out


def _meet(spots):
    barrier = pltpu.get_barrier_semaphore()
    for _, others in spots:
        for other in others:
            pl.semaphore_signal(barrier, device_id={"dp": other}, device_id_type=pl.DeviceIdType.MESH)
    pl.semaphore_wait(barrier, SUMS)


def ring_scratch(steps, chunk):
    two = lambda n, dtype=BF16: pltpu.VMEM((2, SLOTS, 2, n, ROW, LANE), dtype)
    sizes = [n for c in CHUNKS for n in (c // 2, c)]
    kinds = 2 * SUMS if chunk == TILES else 2 * SUMS - 2
    return ([pltpu.VMEM((SLOTS, SLOTS, TILES, ROW, LANE), BF16), pltpu.VMEM((steps, SLOTS, chunk, ROW, LANE), BF16)]
            + [two(n) for n in sizes] + [two(n) for n in sizes[2:]]
            + [pltpu.VMEM((2, SLOTS, n, ROW, LANE), F32) for n in CHUNKS[:2]]
            + [pltpu.SemaphoreType.DMA((kinds, 2, SLOTS, 2))] * 2)


class Ring:
    def __init__(self, steps, chunk, used, refs):
        self.steps, self.whole, self.used, self.spots = steps, chunk == TILES, used, _spots()
        self.kinds = 2 * SUMS if self.whole else 2 * SUMS - 2
        self.grads, self.gathered, *rest = refs
        self.taken, self.staged, self.totals = rest[:SUMS], [None] * 2 + rest[SUMS:-4], rest[-4:-2]
        self.send_sem, self.recv_sem = rest[-2:]

    def copies(self, kind, t, m):
        level, second = divmod(kind, 2)
        level = level if kind < SUMS else 2 * SUMS // 2 - 1 - level
        chain = [self.spots[(m + n) % SLOTS] for n in range(SLOTS)]
        places, devices = chain[level]
        size, slot = CHUNKS[level], _rem(t, 2)
        out = []
        for way in range(2):
            if kind < SUMS:
                if level:
                    src = self.staged[kind].at[slot, m, way]
                elif second:
                    src = self.grads.at[_rem(t, SLOTS), m, pl.ds(size * places[1 + 2 * way], size)]
                else:
                    src = self.grads.at[_rem(t, SLOTS), m, pl.ds(size * places[2] + size // 2 * way, size // 2)]
                dst = self.taken[kind].at[slot, m, way]
            else:
                at = sum(CHUNKS[n] * chain[n][0][0] for n in range(0 if self.whole else 1, level))
                if second:
                    at, size_now = at + size * places[-1 - 2 * way] + size // 2 * way, size // 2
                else:
                    at, size_now = at + (size * places[0] if level or self.whole else 0), size
                src = dst = self.gathered.at[t, m, pl.ds(at, size_now)]
            out.append(pltpu.make_async_remote_copy(src_ref=src, dst_ref=dst, send_sem=self.send_sem.at[kind, slot, m, way],
                                                    recv_sem=self.recv_sem.at[kind, slot, m, way], device_id={"dp": devices[way]},
                                                    device_id_type=pl.DeviceIdType.MESH))
        return out

    def each(self, t, do):
        for m in range(SLOTS):
            if self.used is None:
                do(m)
            else:
                pl.when(self.used(t, m))(functools.partial(do, m))

    def send(self, kind, t):
        self.each(t, lambda m: [copy.start() for copy in self.copies(kind, t, m)] and None)

    def take(self, kind, t):
        def one(m):
            for copy in self.copies(kind, t, m):
                copy.wait_send()
                copy.wait_recv()
            if kind < SUMS:
                self.add(kind, t, m)

        self.each(t, one)

    def add(self, kind, t, m):
        level, second = divmod(kind, 2)
        size, half, slot = CHUNKS[level], CHUNKS[level] // 2, _rem(t, 2)
        chain = [self.spots[(m + n) % SLOTS][0] for n in range(SLOTS)]
        places = chain[level]
        got = [self.taken[kind].at[slot, m, way] for way in range(2)]
        own = self.totals[level - 1].at[slot, m] if level else self.grads.at[_rem(t, SLOTS), m]
        if not second:
            for way in range(2):
                at = size * places[1 + 2 * way]
                joined, alone = pl.ds(at + half * way, half), pl.ds(at + half * (1 - way), half)
                mix = (own[joined].astype(F32) + got[way][...].astype(F32)).astype(BF16)
                if level:
                    send = self.staged[kind + 1].at[slot, m, way]
                    send[pl.ds(half * way, half)] = mix
                    send[pl.ds(half * (1 - way), half)] = own[alone].astype(BF16)
                else:
                    own[joined] = mix
            return
        total = own[pl.ds(size * places[0], size)].astype(F32) + got[0][...].astype(F32) + got[1][...].astype(F32)
        if level + 1 < SLOTS:
            size, half, total_ref = CHUNKS[level + 1], CHUNKS[level + 1] // 2, self.totals[level].at[slot, m]
            total_ref[...] = total
            for way in range(2):
                self.staged[kind + 1][slot, m, way] = total_ref[pl.ds(size * chain[level + 1][2] + half * way, half)].astype(BF16)
        else:
            at = sum(CHUNKS[n] * chain[n][0] for n in range(0 if self.whole else 1, SLOTS))
            self.gathered[t, m, pl.ds(at, size)] = total.astype(BF16)

    def step(self, s, done):
        for kind in reversed(range(self.kinds)):
            t = s - 2 - kind

            @pl.when((t >= 0) & (t < self.steps))
            def _(kind=kind, t=t):
                self.take(kind, t)
                if kind + 1 < self.kinds:
                    self.send(kind + 1, t)
                else:
                    done(t)

        @pl.when((s >= 1) & (s <= self.steps))
        def _():
            self.send(0, s - 1)


def _store(unit, base, part):
    wide = part.shape[1] // LANE
    for r in range(part.shape[0] // ROW):
        for c in range(wide):
            unit[base + r * wide + c] = part[r * ROW : (r + 1) * ROW, c * LANE : (c + 1) * LANE]


TC = 256


def _mlp(steps, h1_ref, dy_ref, wg_ref, wu_ref, wd_ref, out0, out1, out2, dh1_ref, b_s, bt_s, dyt_s, dbg_s, dbu_s, dg_s, du_s, act_s,
         out_sem, *ring_refs):
    step = pl.program_id(0)
    tokens = h1_ref.shape[0]
    ring = Ring(steps, CHUNKS[0], None, ring_refs)

    def out_copies(t):
        return [pltpu.make_async_copy(ring.gathered.at[t, m], out.at[t], out_sem.at[_rem(t, 2), m]) for m, out in enumerate((out0, out1, out2))]

    def done(t):
        for copy in out_copies(t):
            copy.start()

        @pl.when(t > 0)
        def _():
            for copy in out_copies(t - 1):
                copy.wait()

    @pl.when(step == 0)
    def _():
        _meet(ring.spots)
        b = _normed(h1_ref[...])
        b_s[...] = b
        bt_s[...] = b.T
        dyt_s[...] = dy_ref[...].T
        dbg_s[...] = jnp.zeros_like(dbg_s)
        dbu_s[...] = jnp.zeros_like(dbu_s)

    ring.step(step, done)

    @pl.when(step < steps)
    def _():
        def chunk(n, _):
            here = pl.ds(n * TC, TC)
            b, dy = b_s[here, :], dy_ref[here, :]
            gate, up = _nn(b, wg_ref[...]), _nn(b, wu_ref[...])
            dact = _nt(dy, wd_ref[...]).astype(BF16).astype(F32)
            sig = 1 / (1 + jnp.exp(-gate))
            silu = gate * sig
            act_s[here, :] = (silu * up).astype(BF16)
            du = (dact * silu).astype(BF16)
            dg = (dact * up * (sig * (1 + gate * (1 - sig)))).astype(BF16)
            du_s[here, :], dg_s[here, :] = du, dg
            dbg_s[here, :] += _nt(dg, wg_ref[...])
            dbu_s[here, :] += _nt(du, wu_ref[...])
            return _

        lax.fori_loop(0, tokens // TC, chunk, None)
        units = ring.grads.at[_rem(step, SLOTS)]
        _store(units.at[0], 0, _nn(bt_s[...], dg_s[...]).astype(BF16))
        _store(units.at[1], 0, _nn(bt_s[...], du_s[...]).astype(BF16))
        _store(units.at[2], 0, _nn(dyt_s[...], act_s[...]).astype(BF16).T)

    @pl.when(step == steps - 1)
    def _():
        db = (dbg_s[...].astype(BF16) + dbu_s[...].astype(BF16)).astype(F32)
        wide = h1_ref[...].astype(F32)
        scale = lax.rsqrt(jnp.mean(wide * wide, -1, keepdims=True) + 1e-6)
        dot = jnp.sum(db * wide, -1, keepdims=True)
        back = db * scale - wide * (scale * scale * scale * dot * (1 / wide.shape[1]))
        dh1_ref[...] = dy_ref[...] + back.astype(BF16)

    @pl.when(step == pl.num_programs(0) - 1)
    def _():
        for copy in out_copies(steps - 1):
            copy.wait()


def mlp(h1, dy, wg, wu, wd):
    tokens, d = h1.shape
    ff = wg.shape[1]
    steps = ff // FT
    whole = lambda s: (0, 0)
    cols = pl.BlockSpec((d, FT), lambda s: (0, jnp.minimum(s, steps - 1)))
    rows = pl.BlockSpec((FT, d), lambda s: (jnp.minimum(s, steps - 1), 0))
    quarter = jax.ShapeDtypeStruct((steps, CHUNKS[0], ROW, LANE), BF16)
    return pl.pallas_call(
        functools.partial(_mlp, steps),
        grid=(steps + 11,),
        in_specs=[pl.BlockSpec((tokens, d), whole)] * 2 + [cols, cols, rows],
        out_specs=[pl.BlockSpec(memory_space=pl.ANY)] * 3 + [pl.BlockSpec((tokens, d), whole)],
        out_shape=[quarter] * 3 + [jax.ShapeDtypeStruct((tokens, d), BF16)],
        scratch_shapes=[pltpu.VMEM((tokens, d), BF16), pltpu.VMEM((d, tokens), BF16), pltpu.VMEM((d, tokens), BF16)]
        + [pltpu.VMEM((tokens, d), F32)] * 2 + [pltpu.VMEM((tokens, FT), BF16)] * 3 + [pltpu.SemaphoreType.DMA((2, 3))]
        + ring_scratch(steps, CHUNKS[0]),
        compiler_params=pltpu.CompilerParams(dimension_semantics=("arbitrary",), vmem_limit_bytes=VMEM, collective_id=0, has_side_effects=True),
        cost_estimate=pl.CostEstimate(flops=16 * tokens * d * ff, transcendentals=tokens * ff, bytes_accessed=60 * 10**6),
        name="mlp",
    )(h1, dy, wg, wu, wd)


def _attn_bwd(steps, h_ref, dh1_ref, cos_ref, sin_ref, q_ref, k_ref, v_ref, ot_ref, lse_ref, wo_ref, out_ref,
              at_s, dq_s, dk_s, dv_s, out_sem, *ring_refs):
    step = pl.program_id(0)
    tokens = h_ref.shape[0]
    scale = HEAD**-0.5
    e = scale * LOG2E
    slot_of = lambda t, j: _rem(2 * t + j, SLOTS)
    ring = Ring(steps, TILES, lambda t, m: slot_of(t, 2) != m, ring_refs)

    def out_copy(t):
        return pltpu.make_async_copy(ring.gathered.at[t], out_ref.at[t], out_sem.at[_rem(t, 2)])

    def done(t):
        out_copy(t).start()

        @pl.when(t > 0)
        def _():
            out_copy(t - 1).wait()

    @pl.when(step == 0)
    def _():
        _meet(ring.spots)
        at_s[...] = _normed(h_ref[...]).T

    ring.step(step, done)

    @pl.when(step < steps)
    def _():
        d_out = _nt(dh1_ref[...], wo_ref[...]).astype(BF16)
        units = [ring.grads.at[_rem(step, SLOTS), slot_of(step, j)] for j in range(2)]

        def keep(matrix, both):
            for j in range(2):
                part = both[:, j * HEAD : (j + 1) * HEAD] if matrix < 3 else both[j * HEAD : (j + 1) * HEAD]
                _store(units[j], CHUNKS[0] * matrix, part)

        keep(3, _nn(ot_ref[...], dh1_ref[...]).astype(BF16))
        seen = lax.broadcasted_iota(jnp.int32, (QB, QB), 0) <= lax.broadcasted_iota(jnp.int32, (QB, QB), 1)
        for j in range(PAIR // HEAD):
            cols = slice(j * HEAD, (j + 1) * HEAD)
            kt = k_ref[:, cols].T
            for i in reversed(range(tokens // QB)):
                end = (i + 1) * QB
                q, do = q_ref[i * QB : end, cols], d_out[i * QB : end, cols]
                lse = lse_ref[pl.ds(step * 2 + j, 1), i * QB : end] * LOG2E
                p = jnp.exp2(_nt(k_ref[:end, cols], q) * e - lse)
                last = jnp.where(seen, p[i * QB :], 0.0)
                p = jnp.concatenate([p[: i * QB], last], axis=0) if i else last
                dp = _nt(v_ref[:end, cols], do)
                both = p * dp
                ds = (both - p * both.sum(axis=0, keepdims=True)).astype(BF16)
                dv, dk = _nn(p.astype(BF16), do), _nn(ds, q)
                if end == tokens:
                    dv_s[:, cols], dk_s[:, cols] = dv, dk
                else:
                    dv_s[:end, cols] += dv
                    dk_s[:end, cols] += dk
                dq_s[i * QB : end, cols] = _nn(kt[:, :end], ds).T
        at = at_s[...]
        for matrix, g_s in enumerate((dq_s, dk_s)):
            turned = []
            for j in range(PAIR // HEAD):
                g = (g_s[:, j * HEAD : (j + 1) * HEAD] * scale).astype(BF16).astype(F32)
                turned.append((g * cos_ref[...] - pltpu.roll(g, HEAD // 2, 1) * sin_ref[...]).astype(BF16))
            keep(matrix, _nn(at, jnp.concatenate(turned, axis=1)).astype(BF16))
        keep(2, _nn(at, dv_s[...].astype(BF16)).astype(BF16))

    @pl.when(step == pl.num_programs(0) - 1)
    def _():
        out_copy(steps - 1).wait()


def attn_bwd(h, dh1, cos, sin, q, k, v, ot, lse, wo):
    tokens, d = h.shape
    width = q.shape[1]
    steps = width // PAIR
    whole = lambda s: (0, 0)
    cols = lambda s: (0, jnp.minimum(s, steps - 1))
    rows = lambda s: (jnp.minimum(s, steps - 1), 0)
    return pl.pallas_call(
        functools.partial(_attn_bwd, steps),
        grid=(steps + 13,),
        in_specs=[pl.BlockSpec((tokens, d), whole)] * 2 + [pl.BlockSpec((tokens, HEAD), whole)] * 2 + [pl.BlockSpec((tokens, PAIR), cols)] * 3
        + [pl.BlockSpec((PAIR, tokens), rows), pl.BlockSpec((width // HEAD, tokens), whole), pl.BlockSpec((PAIR, d), rows)],
        out_specs=pl.BlockSpec(memory_space=pl.ANY),
        out_shape=jax.ShapeDtypeStruct((steps, SLOTS, TILES, ROW, LANE), BF16),
        scratch_shapes=[pltpu.VMEM((d, tokens), BF16)] + [pltpu.VMEM((tokens, PAIR), F32)] * 3 + [pltpu.SemaphoreType.DMA((2,))]
        + ring_scratch(steps, TILES),
        compiler_params=pltpu.CompilerParams(dimension_semantics=("arbitrary",), vmem_limit_bytes=VMEM, collective_id=1, has_side_effects=True),
        cost_estimate=pl.CostEstimate(flops=30 * 10**9, transcendentals=10**7, bytes_accessed=40 * 10**6),
        name="attn_bwd",
    )(h, dh1, cos, sin, q, k, v, ot, lse, wo)


def angles(tokens):
    half = HEAD // 2
    angle = jnp.arange(tokens, dtype=F32)[:, None] * THETA ** (-jnp.arange(half, dtype=F32) / half)
    cos, sin = jnp.cos(angle), jnp.sin(angle)
    return jnp.concatenate([cos, cos], -1), jnp.concatenate([-sin, sin], -1)


def _adamw(w, m, v, g):
    m = 0.9 * m + 0.1 * g
    v = 0.95 * v + 0.05 * g * g
    step = m * lax.rsqrt(v + 1e-8) + 0.1 * w
    return (w - 0.02 * step).astype(BF16), m, v


def _update(g_tile, old, new, wide, rows):
    def band(r, _):
        at = pl.ds(pl.multiple_of(r * ROW, ROW), ROW)
        for b in range(len(old)):
            for c in range(wide):
                lanes = slice(c * LANE, (c + 1) * LANE)
                (w, m, v), (w_new, m_new, v_new) = old[b], new[b]
                w_new[at, lanes], m_new[at, lanes], v_new[at, lanes] = _adamw(
                    w[at, lanes].astype(F32), m[at, lanes], v[at, lanes], g_tile(b, r, c).astype(F32))
        return _

    lax.fori_loop(0, rows // ROW, band, None)


BLOCKS = 4
MATRICES = 3


def _mlp_update(pieces, table_ref, *refs):
    n = MATRICES * (3 if pieces else 2)
    g_refs, old, new = refs[:n], refs[n : n + 9], refs[-9:]

    def views(three, tall):
        return [[(x.at[b, 0] if tall else x.at[0, :, pl.ds(b * FT, FT)]) for x in three] for b in range(BLOCKS)]

    for c in range(MATRICES):
        mine, olds, news = g_refs[c::MATRICES], *(views(x[3 * c : 3 * c + 3], c == 2) for x in (old, new))
        if pieces:
            for q in range(3):

                @pl.when(pl.program_id(0) == q)
                def _(q=q):
                    _update(lambda b, r, k: mine[q][b, r * SIDE + k], olds, news, SIDE, LANE)
        else:
            rows = LANE // 2
            for half in range(2):
                olds_now, news_now = ([[x.at[pl.ds(rows * half, rows)] for x in block] for block in all_] for all_ in (olds, news))
                _update(lambda b, r, k: mine[half][b, r * SIDE + k], olds_now, news_now, SIDE, rows)


def mlp_update(tables, gradient, old, so_far):
    pieces = so_far is None
    blocks = gradient[0].shape[0] // BLOCKS
    last = blocks - 1
    grid = (3, blocks) if pieces else (1, blocks)
    views, spots = [], []
    for c, w in enumerate(old[::3]):
        rows, columns = w.shape
        if c == 2:
            views.append((rows // FT, SIDE, LANE, columns))
            spots.append(pl.BlockSpec((BLOCKS, 1, LANE, columns), lambda q, b, t, c=c: (b, t[c, q], 0, 0)))
        else:
            views.append((SIDE, LANE, columns))
            spots.append(pl.BlockSpec((1, LANE, BLOCKS * FT), lambda q, b, t, c=c: (t[c, q], 0, b)))
    g_specs = [pl.BlockSpec((BLOCKS, *g.shape[1:]),
                            lambda q, b, t, n=n: (jnp.where(q == n, b, jnp.where(q < n, 0, last)) if pieces else b, 0, 0, 0))
               for n, g in zip([k // MATRICES for k in range(len(gradient))], gradient)]
    all_views, all_spots = ([x for x in xs for _ in range(3)] for xs in (views, spots))
    given = [x.reshape(view) for x, view in zip(old, all_views)]
    kept = [] if pieces else so_far
    first = 1 + len(gradient) + len(given)
    return pl.pallas_call(
        functools.partial(_mlp_update, pieces),
        grid_spec=pltpu.PrefetchScalarGridSpec(
            num_scalar_prefetch=1, grid=grid, in_specs=g_specs + all_spots + [pl.BlockSpec(memory_space=pl.ANY)] * len(kept), out_specs=all_spots),
        out_shape=[jax.ShapeDtypeStruct(x.shape, x.dtype) for x in given],
        input_output_aliases={first + n: n for n in range(len(kept))},
        compiler_params=pltpu.CompilerParams(dimension_semantics=("arbitrary",) * 2, vmem_limit_bytes=VMEM),
        cost_estimate=pl.CostEstimate(flops=sum(g.size for g in gradient) * 16, transcendentals=0, bytes_accessed=sum(g.size for g in gradient) * 22),
        name="mlp_update",
    )(tables, *gradient, *given, *kept)


def _attn_update(g_ref, *refs):
    old, new = refs[: len(refs) // 2], refs[len(refs) // 2 :]
    heads = PAIR // HEAD
    for n in range(4):
        wide, rows = (1, 512) if n < 3 else (SIDE, HEAD)
        view = lambda x, j: x.at[:, pl.ds(j * HEAD, HEAD)] if n < 3 else x.at[pl.ds(j * HEAD, HEAD)]
        olds, news = ([[view(x, j) for x in xs[3 * n : 3 * n + 3]] for j in range(heads)] for xs in (old, new))
        slots = [_rem(heads * pl.program_id(0) + j, SLOTS) for j in range(heads)]
        _update(lambda b, r, c: g_ref[0, slots[b], CHUNKS[0] * n + r * wide + c], olds, news, wide, rows)


def attn_update(gradient, old):
    steps = gradient.shape[0]
    d = old[0].shape[0]
    specs = [pl.BlockSpec((d, PAIR), lambda s: (0, s))] * 9 + [pl.BlockSpec((PAIR, d), lambda s: (s, 0))] * 3
    return pl.pallas_call(
        _attn_update,
        grid=(steps,),
        in_specs=[pl.BlockSpec((1, *gradient.shape[1:]), lambda s: (s, 0, 0, 0, 0))] + specs,
        out_specs=specs,
        out_shape=[jax.ShapeDtypeStruct(x.shape, x.dtype) for x in old],
        compiler_params=pltpu.CompilerParams(dimension_semantics=("arbitrary",), vmem_limit_bytes=VMEM),
        cost_estimate=pl.CostEstimate(flops=gradient.size * 16, transcendentals=0, bytes_accessed=gradient.size * 22),
        name="attn_update",
    )(gradient, *old)


def shifted(axis, by):
    stride = SIDE ** (2 - axis)
    return [(d, d + ((d // stride % SIDE + by) % SIDE - d // stride % SIDE) * stride) for d in range(SIDE**3)]


def solution(mesh):
    def step(x, dy, *arrays):
        weights, m, v = ([a[0] for a in arrays[i : i + 7]] for i in (0, 7, 14))
        old = [a for three in zip(weights, m, v) for a in three]
        h = x[0]
        wq, wk, wv, wo, wg, wu, wd = weights
        axes = range(MATRICES)
        cos, sin = angles(h.shape[0])
        q, k, v_, ot, lse, h1 = attn_fwd(h, cos, sin, wq, wk, wv, wo)
        *own, dh1 = mlp(h1, dy[0], wg, wu, wd)
        back = [lax.ppermute(own[c], "dp", shifted(c, 1)) for c in axes]
        ahead = [lax.ppermute(own[c], "dp", shifted(c, -1)) for c in axes]
        attn = attn_bwd(h, dh1, cos, sin, q, k, v_, ot, lse, wo)
        half = CHUNKS[0] // 2
        first = [lax.ppermute(back[c][:, :half], "dp", shifted(c, 1)) for c in axes]
        second = [lax.ppermute(ahead[c][:, half:], "dp", shifted(c, -1)) for c in axes]
        places = jnp.stack([places[0] for places, _ in _spots()])
        table = lambda *away: (places[:, None] + jnp.array(away, jnp.int32)) % SIDE
        new = mlp_update(table(0, 3, 1), own + back + ahead, old[12:], None)
        new = mlp_update(table(2), first + second, old[12:], new)
        new = [*attn_update(attn, old[:12])] + [a.reshape(b.shape) for a, b in zip(new, old[12:])]
        return tuple(a[None] for which in range(3) for a in new[which::3])

    states, all_of = P(("rep", "dp"), None, None), P(None, None, None)
    return jax.shard_map(
        step,
        mesh=mesh,
        in_specs=(states, states) + (all_of,) * 21,
        out_specs=(P("rep", None, None),) * 21,
        check_vma=False,
    )
```

```python
import functools

import jax
import jax.numpy as jnp
from jax import lax
from jax.experimental import pallas as pl
from jax.experimental.pallas import tpu as pltpu
from jax.sharding import PartitionSpec as P

HEAD = 128
THETA = 10000
LOG2E = 1.4426950408889634
HIDDEN = -1e30
VMEM = 60 * 2**20
F32, BF16 = jnp.float32, jnp.bfloat16
QB = 512
PAIR = 256
FT = 512


def _nn(a, b):
    return lax.dot_general(a, b, (((1,), (0,)), ((), ())), preferred_element_type=F32)


def _nt(a, b):
    return lax.dot_general(a, b, (((1,), (1,)), ((), ())), preferred_element_type=F32)


def _tn(a, b):
    return lax.dot_general(a, b, (((0,), (0,)), ((), ())), preferred_element_type=F32)


def _normed(h):
    wide = h.astype(F32)
    scale = lax.rsqrt(jnp.mean(wide * wide, -1, keepdims=True) + 1e-6)
    return (wide * scale).astype(BF16)


def _attn_fwd(h_ref, cos_ref, sin_ref, wq_ref, wk_ref, wv_ref, wo_ref, q_ref, k_ref, v_ref, ot_ref, lse_ref, h1_ref, a_s, ot_s):
    step = pl.program_id(0)
    tokens = h_ref.shape[0]
    scale = HEAD**-0.5
    e = scale * LOG2E

    @pl.when(step == 0)
    def _():
        a_s[...] = _normed(h_ref[...])

    a = a_s[...]
    for w_ref, o_ref in ((wq_ref, q_ref), (wk_ref, k_ref)):
        t = _nn(a, w_ref[...]).astype(BF16).astype(F32)
        for j in range(PAIR // HEAD):
            one = t[:, j * HEAD : (j + 1) * HEAD]
            o_ref[:, j * HEAD : (j + 1) * HEAD] = (one * cos_ref[...] + pltpu.roll(one, HEAD // 2, 1) * sin_ref[...]).astype(BF16)
    v_ref[...] = _nn(a, wv_ref[...]).astype(BF16)

    seen = lax.broadcasted_iota(jnp.int32, (QB, QB), 0) <= lax.broadcasted_iota(jnp.int32, (QB, QB), 1)
    work = []
    for j in range(PAIR // HEAD):
        cols = slice(j * HEAD, (j + 1) * HEAD)
        for i in range(tokens // QB):
            end = (i + 1) * QB
            q = q_ref[i * QB : end, cols]
            parts = [_nt(k_ref[: i * QB, cols], q)] if i else []
            work.append((j, i, parts + [_nt(k_ref[i * QB : end, cols], q)]))
    for j, i, parts in work:
        cols, end = slice(j * HEAD, (j + 1) * HEAD), (i + 1) * QB
        parts = parts[:-1] + [jnp.where(seen, parts[-1], HIDDEN)]
        top = functools.reduce(jnp.maximum, [s.max(axis=0, keepdims=True) for s in parts])
        weights = [jnp.exp2((s - top) * e) for s in parts]
        total = sum(w.sum(axis=0, keepdims=True) for w in weights)
        p = jnp.concatenate([w.astype(BF16) for w in weights], axis=0)
        o = (_nn(v_ref[:end, cols].T, p) * (1 / total)).astype(BF16)
        ot_ref[cols, i * QB : end] = o
        ot_s[pl.ds(step * PAIR + j * HEAD, HEAD), i * QB : end] = o
        lse_ref[pl.ds(step * 2 + j, 1), i * QB : end] = top * scale + jnp.log(total)

    @pl.when(step == pl.num_programs(0) - 1)
    def _():
        mixed = _tn(wo_ref[...], ot_s[...]).astype(BF16).T
        h1_ref[...] = h_ref[...] + mixed


def attn_fwd(h, cos, sin, wq, wk, wv, wo):
    tokens, d = h.shape
    width = wq.shape[1]
    whole = lambda s: (0, 0)
    cols = lambda s: (0, s)
    return pl.pallas_call(
        _attn_fwd,
        grid=(width // PAIR,),
        in_specs=[pl.BlockSpec((tokens, d), whole), pl.BlockSpec((tokens, HEAD), whole), pl.BlockSpec((tokens, HEAD), whole)]
        + [pl.BlockSpec((d, PAIR), cols)] * 3 + [pl.BlockSpec((width, d), whole)],
        out_specs=[pl.BlockSpec((tokens, PAIR), cols)] * 3 + [pl.BlockSpec((PAIR, tokens), lambda s: (s, 0)),
                   pl.BlockSpec((width // HEAD, tokens), whole), pl.BlockSpec((tokens, d), whole)],
        out_shape=[jax.ShapeDtypeStruct((tokens, width), BF16)] * 3 + [jax.ShapeDtypeStruct((width, tokens), BF16),
                   jax.ShapeDtypeStruct((width // HEAD, tokens), F32), jax.ShapeDtypeStruct((tokens, d), BF16)],
        scratch_shapes=[pltpu.VMEM((tokens, d), BF16), pltpu.VMEM((width, tokens), BF16)],
        compiler_params=pltpu.CompilerParams(dimension_semantics=("arbitrary",), vmem_limit_bytes=VMEM),
        cost_estimate=pl.CostEstimate(flops=20 * 10**9, transcendentals=10**7, bytes_accessed=40 * 10**6),
        name="attn_fwd",
    )(h, cos, sin, wq, wk, wv, wo)


ROW, LANE, TILES, SIDE, SLOTS = 16, 128, 128, 4, 3
CHUNKS = (32, 8, 2)
SUMS = 6
KINDS = 2 * SUMS
NEAR = KINDS - 2
DELAY = 1
TURNS = 2 * DELAY


def _rem(a, n):
    return lax.rem(a, jnp.int32(n))


def _spots():
    d = lax.axis_index("dp")
    out = []
    for stride in (SIDE * SIDE, SIDE, 1):
        places = [_rem(lax.div(d, jnp.int32(stride)) + n, SIDE) for n in range(SIDE)]
        out.append((places, [d + (places[n] - places[0]) * stride for n in (1, -1)]))
    return out


def _meet(spots):
    barrier = pltpu.get_barrier_semaphore()
    for _, others in spots:
        for other in others:
            pl.semaphore_signal(barrier, device_id={"dp": other}, device_id_type=pl.DeviceIdType.MESH)


def _met():
    pl.semaphore_wait(pltpu.get_barrier_semaphore(), SUMS)


def ring_scratch(steps):
    turns = lambda n: pltpu.VMEM((TURNS, SLOTS, 2, n, ROW, LANE), BF16)
    sizes = [n for c in CHUNKS for n in (c // 2, c)]
    return ([pltpu.VMEM((TURNS + 2, SLOTS, TILES, ROW, LANE), BF16), pltpu.VMEM((steps, SLOTS, CHUNKS[0], ROW, LANE), BF16)]
            + [turns(n) for n in sizes] + [turns(n) for n in sizes[2:]]
            + [pltpu.VMEM((TURNS, SLOTS, n, ROW, LANE), F32) for n in CHUNKS[:2]]
            + [pltpu.SemaphoreType.DMA((KINDS, TURNS, SLOTS, 2))] * 2)


class Ring:
    def __init__(self, steps, first_whole, whole, used, refs):
        self.steps, self.first_whole, self.whole, self.used, self.spots = steps, first_whole, whole, used, _spots()
        self.grads, self.gathered, *rest = refs
        self.taken, self.staged, self.totals = rest[:SUMS], [None] * 2 + rest[SUMS:-4], rest[-4:-2]
        self.send_sem, self.recv_sem = rest[-2:]

    def unit(self, t):
        return self.grads.at[_rem(t, TURNS + 2)]

    def copies(self, kind, t, m):
        level, second = divmod(kind, 2)
        level = level if kind < SUMS else SUMS - 1 - level
        chain = [self.spots[(m + n) % SLOTS] for n in range(SLOTS)]
        places, devices = chain[level]
        size, slot = CHUNKS[level], _rem(t, TURNS)
        out = []
        for way in range(2):
            if kind < SUMS:
                if level:
                    src = self.staged[kind].at[slot, m, way]
                elif second:
                    src = self.unit(t).at[m, pl.ds(size * places[1 + 2 * way], size)]
                else:
                    src = self.unit(t).at[m, pl.ds(size * places[2] + size // 2 * way, size // 2)]
                dst = self.taken[kind].at[slot, m, way]
            else:
                held = self.gathered.at[t, m] if level else self.whole.at[t - self.first_whole, m]
                at, n = sum(CHUNKS[n] * chain[n][0][0] for n in range(1, level)), size
                if second:
                    at, n = at + size * places[-1 - 2 * way] + size // 2 * way, size // 2
                else:
                    at = at + size * places[0]
                src = dst = held.at[pl.ds(at, n)]
                if kind == NEAR:
                    src = self.gathered.at[t, m]
            out.append(pltpu.make_async_remote_copy(src_ref=src, dst_ref=dst, send_sem=self.send_sem.at[kind, slot, m, way],
                                                    recv_sem=self.recv_sem.at[kind, slot, m, way], device_id={"dp": devices[way]},
                                                    device_id_type=pl.DeviceIdType.MESH))
        return out

    def each(self, t, do):
        for m in range(SLOTS):
            pl.when(self.used(t, m))(functools.partial(do, m))

    def send(self, kind, t):
        self.each(t, lambda m: [copy.start() for copy in self.copies(kind, t, m)] and None)

    def take(self, kind, t):
        def one(m):
            for copy in self.copies(kind, t, m):
                copy.wait_send()
                copy.wait_recv()
            if kind < SUMS:
                self.add(kind, t, m)

        self.each(t, one)

    def add(self, kind, t, m):
        level, second = divmod(kind, 2)
        size, half, slot = CHUNKS[level], CHUNKS[level] // 2, _rem(t, TURNS)
        chain = [self.spots[(m + n) % SLOTS][0] for n in range(SLOTS)]
        places = chain[level]
        got = [self.taken[kind].at[slot, m, way] for way in range(2)]
        own = self.totals[level - 1].at[slot, m] if level else self.unit(t).at[m]
        if not second:
            for way in range(2):
                at = size * places[1 + 2 * way]
                joined, alone = pl.ds(at + half * way, half), pl.ds(at + half * (1 - way), half)
                mix = (own[joined].astype(F32) + got[way][...].astype(F32)).astype(BF16)
                if level:
                    send = self.staged[kind + 1].at[slot, m, way]
                    send[pl.ds(half * way, half)] = mix
                    send[pl.ds(half * (1 - way), half)] = own[alone].astype(BF16)
                else:
                    own[joined] = mix
            return
        total = own[pl.ds(size * places[0], size)].astype(F32) + got[0][...].astype(F32) + got[1][...].astype(F32)
        if level + 1 < SLOTS:
            size, half, total_ref = CHUNKS[level + 1], CHUNKS[level + 1] // 2, self.totals[level].at[slot, m]
            total_ref[...] = total
            for way in range(2):
                self.staged[kind + 1][slot, m, way] = total_ref[pl.ds(size * chain[level + 1][2] + half * way, half)].astype(BF16)
        else:
            self.gathered[t, m, pl.ds(sum(CHUNKS[n] * chain[n][0] for n in range(1, SLOTS)), size)] = total.astype(BF16)

    def step(self, s, kept):
        for kind in reversed(range(KINDS)):
            t = s - 1 - DELAY * (kind + 1)
            far = kind + 1 >= NEAR

            @pl.when((t >= (self.first_whole if kind >= NEAR else 0)) & (t < self.steps))
            def _(kind=kind, t=t, far=far):
                self.take(kind, t)
                if kind + 1 == NEAR:
                    kept(t)
                if kind + 1 < KINDS:
                    pl.when(t >= (self.first_whole if far else 0))(lambda: self.send(kind + 1, t))

        @pl.when((s >= 1) & (s <= self.steps))
        def _():
            self.send(0, s - 1)


def _store(unit, base, part):
    wide = part.shape[1] // LANE
    for r in range(part.shape[0] // ROW):
        for c in range(wide):
            unit[base + r * wide + c] = part[r * ROW : (r + 1) * ROW, c * LANE : (c + 1) * LANE]


def _mlp_step(b_s, bt_s, dy_ref, dyt_s, wg_ref, wu_ref, wd_ref, dbg_s, dbu_s, dg_s, du_s, act_s, units):
    halves = [slice(i * FT // 2, (i + 1) * FT // 2) for i in range(2)]
    b, dy = b_s[...], dy_ref[...]
    made = [(_nn(b, wg_ref[:, at]), _nn(b, wu_ref[:, at]), _nt(dy, wd_ref[at, :])) for at in halves]
    for at, (gate, up, dact) in zip(halves, made):
        dact = dact.astype(BF16).astype(F32)
        sig = 1 / (1 + jnp.exp(-gate))
        silu = gate * sig
        act_s[:, at] = (silu * up).astype(BF16)
        du_s[:, at] = (dact * silu).astype(BF16)
        dg_s[:, at] = (dact * up * (sig * (1 + gate * (1 - sig)))).astype(BF16)
    _store(units.at[0], 0, _nn(bt_s[...], dg_s[...]).astype(BF16))
    _store(units.at[1], 0, _nn(bt_s[...], du_s[...]).astype(BF16))
    _store(units.at[2], 0, _nn(dyt_s[...], act_s[...]).astype(BF16).T)
    dbg_s[...] += _nt(dg_s[...], wg_ref[...])
    dbu_s[...] += _nt(du_s[...], wu_ref[...])


def _attn_step(n, at_s, dh1_s, cos_ref, sin_ref, q_ref, k_ref, v_ref, ot_ref, lse_ref, wo_ref, dq_s, dk_s, dv_s, units):
    tokens = dh1_s.shape[0]
    scale = HEAD**-0.5
    e = scale * LOG2E
    heads = PAIR // HEAD

    def keep(matrix, both):
        for j in range(heads):
            part = both[:, j * HEAD : (j + 1) * HEAD] if matrix < 3 else both[j * HEAD : (j + 1) * HEAD]
            _store(units[j], CHUNKS[0] * matrix, part)

    d_out = _nt(dh1_s[...], wo_ref[...]).astype(BF16)
    keep(3, _nn(ot_ref[...], dh1_s[...]).astype(BF16))
    seen = lax.broadcasted_iota(jnp.int32, (QB, QB), 0) <= lax.broadcasted_iota(jnp.int32, (QB, QB), 1)
    for j in range(heads):
        cols = slice(j * HEAD, (j + 1) * HEAD)
        kt = k_ref[:, cols].T
        for i in reversed(range(tokens // QB)):
            end = (i + 1) * QB
            q, do = q_ref[i * QB : end, cols], d_out[i * QB : end, cols]
            lse = lse_ref[pl.ds(n * heads + j, 1), i * QB : end] * LOG2E
            p = jnp.exp2(_nt(k_ref[:end, cols], q) * e - lse)
            last = jnp.where(seen, p[i * QB :], 0.0)
            p = jnp.concatenate([p[: i * QB], last], axis=0) if i else last
            dp = _nt(v_ref[:end, cols], do)
            both = p * dp
            ds = (both - p * both.sum(axis=0, keepdims=True)).astype(BF16)
            dv, dk = _nn(p.astype(BF16), do), _nn(ds, q)
            if end == tokens:
                dv_s[:, cols], dk_s[:, cols] = dv, dk
            else:
                dv_s[:end, cols] += dv
                dk_s[:end, cols] += dk
            dq_s[i * QB : end, cols] = _nn(kt[:, :end], ds).T
    at = at_s[...]
    for matrix, g_s in enumerate((dq_s, dk_s)):
        turned = []
        for j in range(heads):
            g = (g_s[:, j * HEAD : (j + 1) * HEAD] * scale).astype(BF16).astype(F32)
            turned.append((g * cos_ref[...] - pltpu.roll(g, HEAD // 2, 1) * sin_ref[...]).astype(BF16))
        keep(matrix, _nn(at, jnp.concatenate(turned, axis=1)).astype(BF16))
    keep(2, _nn(at, dv_s[...].astype(BF16)).astype(BF16))


def _backward(mlp_steps, attn_steps, h1_ref, dy_ref, wg_ref, wu_ref, wd_ref, h_ref, cos_ref, sin_ref, q_ref, k_ref, v_ref, ot_ref, lse_ref, wo_ref,
              *refs):
    outs, attn_ref, (b_s, bt_s, dyt_s, dbg_s, dbu_s, dg_s, du_s, act_s, dh1_s, out_sem, *ring_refs) = refs[:SLOTS], refs[SLOTS], refs[SLOTS + 1 :]
    step = pl.program_id(0)
    heads = PAIR // HEAD
    groups = attn_ref.shape[0]
    steps = mlp_steps + groups
    ring = Ring(steps, mlp_steps, attn_ref, lambda t, m: (t < steps - 1) | (m == 0), ring_refs)

    def keep(t, do):
        for m in range(SLOTS):
            copy = lambda dst: pltpu.make_async_copy(ring.gathered.at[t, m], dst, out_sem.at[_rem(t, 2), m])
            pl.when(t < mlp_steps)(lambda: do(copy(outs[m].at[t])))
            pl.when((t >= mlp_steps) & ring.used(t, m))(
                lambda: do(copy(attn_ref.at[t - mlp_steps, m, pl.ds(CHUNKS[0] * ring.spots[m][0][0], CHUNKS[0])])))

    def kept(t):
        keep(t, lambda copy: copy.start())
        pl.when(t > 0)(lambda: keep(t - 1, lambda copy: copy.wait()))

    @pl.when(step == 0)
    def _():
        _meet(ring.spots)
        b = _normed(h1_ref[...])
        b_s[...] = b
        bt_s[...] = b.T
        dyt_s[...] = dy_ref[...].T
        dbg_s[...] = jnp.zeros_like(dbg_s)
        dbu_s[...] = jnp.zeros_like(dbu_s)

    pair = jnp.maximum(step - mlp_steps, 0)
    turn = jnp.minimum(step, mlp_steps) + lax.div(heads * pair + 1, jnp.int32(SLOTS))

    pl.when(step == 1)(_met)

    @pl.when((step < mlp_steps + attn_steps) & (_rem(pair, SLOTS) != 1))
    def _():
        ring.step(turn, kept)

    @pl.when(step < mlp_steps)
    def _():
        _mlp_step(b_s, bt_s, dy_ref, dyt_s, wg_ref, wu_ref, wd_ref, dbg_s, dbu_s, dg_s, du_s, act_s, ring.unit(step))

    @pl.when(step == mlp_steps - 1)
    def _():
        db = (dbg_s[...].astype(BF16) + dbu_s[...].astype(BF16)).astype(F32)
        wide = h1_ref[...].astype(F32)
        scale = lax.rsqrt(jnp.mean(wide * wide, -1, keepdims=True) + 1e-6)
        dot = jnp.sum(db * wide, -1, keepdims=True)
        back = db * scale - wide * (scale * scale * scale * dot * (1 / wide.shape[1]))
        dh1_s[...] = dy_ref[...] + back.astype(BF16)
        bt_s[...] = _normed(h_ref[...]).T

    @pl.when((step >= mlp_steps) & (step < mlp_steps + attn_steps))
    def _():
        units = [ring.unit(mlp_steps + lax.div(n, jnp.int32(SLOTS))).at[_rem(n, SLOTS)] for n in (heads * pair + j for j in range(heads))]
        parts = (dbg_s.at[:, :PAIR], dbg_s.at[:, PAIR:], dbu_s.at[:, :PAIR])
        _attn_step(pair, bt_s, dh1_s, cos_ref, sin_ref, q_ref, k_ref, v_ref, ot_ref, lse_ref, wo_ref, *parts, units)

    @pl.when(step == mlp_steps + attn_steps)
    def _():
        lax.fori_loop(steps - 1, steps + 1 + DELAY * KINDS, lambda n, _: ring.step(n, kept), None)
        keep(steps - 1, lambda copy: copy.wait())


def backward(h, h1, dy, wg, wu, wd, cos, sin, q, k, v, ot, lse, wo):
    tokens, d = h1.shape
    ff, width = wg.shape[1], q.shape[1]
    mlp_steps, attn_steps, groups = ff // FT, width // PAIR, pl.cdiv(width // HEAD, SLOTS)
    one = lambda *shape: pl.BlockSpec(shape, lambda s: (0, 0), pipeline_mode=pl.Buffered(1))
    at = lambda s: jnp.minimum(s, mlp_steps - 1)
    then = lambda s: jnp.clip(s - mlp_steps, 0, attn_steps - 1)
    cols, rows = pl.BlockSpec((d, FT), lambda s: (0, at(s))), pl.BlockSpec((FT, d), lambda s: (at(s), 0))
    heads = pl.BlockSpec((tokens, PAIR), lambda s: (0, then(s)))
    pairs = lambda n: pl.BlockSpec((PAIR, n), lambda s: (then(s), 0))
    quarter = jax.ShapeDtypeStruct((mlp_steps, CHUNKS[0], ROW, LANE), BF16)
    return pl.pallas_call(
        functools.partial(_backward, mlp_steps, attn_steps),
        grid=(mlp_steps + attn_steps + 1,),
        in_specs=[one(tokens, d)] * 2 + [cols, cols, rows] + [one(tokens, d)] + [one(tokens, HEAD)] * 2 + [heads] * 3
        + [pairs(tokens), one(width // HEAD, tokens), pairs(d)],
        out_specs=[pl.BlockSpec(memory_space=pl.ANY)] * (SLOTS + 1),
        out_shape=[quarter] * SLOTS + [jax.ShapeDtypeStruct((groups, SLOTS, TILES, ROW, LANE), BF16)],
        scratch_shapes=[pltpu.VMEM((tokens, d), BF16)] + [pltpu.VMEM((d, tokens), BF16)] * 2 + [pltpu.VMEM((tokens, d), F32)] * 2
        + [pltpu.VMEM((tokens, FT), BF16)] * 3 + [pltpu.VMEM((tokens, d), BF16), pltpu.SemaphoreType.DMA((2, SLOTS))]
        + ring_scratch(mlp_steps + groups),
        compiler_params=pltpu.CompilerParams(dimension_semantics=("arbitrary",), vmem_limit_bytes=VMEM, collective_id=0, has_side_effects=True),
        cost_estimate=pl.CostEstimate(flops=16 * tokens * d * ff, transcendentals=tokens * ff, bytes_accessed=ff * d * 6),
        name="backward",
    )(h1, dy, wg, wu, wd, h, cos, sin, q, k, v, ot, lse, wo)


def angles(tokens):
    half = HEAD // 2
    angle = jnp.arange(tokens, dtype=F32)[:, None] * THETA ** (-jnp.arange(half, dtype=F32) / half)
    cos, sin = jnp.cos(angle), jnp.sin(angle)
    return jnp.concatenate([cos, cos], -1), jnp.concatenate([-sin, sin], -1)


def _adamw(w, m, v, g):
    m = 0.9 * m + 0.1 * g
    v = 0.95 * v + 0.05 * g * g
    step = m * lax.rsqrt(v + 1e-8) + 0.1 * w
    return (w - 0.02 * step).astype(BF16), m, v


def _update(g_tile, old, new, wide, rows):
    def band(r, _):
        at = pl.ds(pl.multiple_of(r * ROW, ROW), ROW)
        for b in range(len(old)):
            for c in range(wide):
                lanes = slice(c * LANE, (c + 1) * LANE)
                (w, m, v), (w_new, m_new, v_new) = old[b], new[b]
                w_new[at, lanes], m_new[at, lanes], v_new[at, lanes] = _adamw(
                    w[at, lanes].astype(F32), m[at, lanes], v[at, lanes], g_tile(b, r, c).astype(F32))
        return _

    lax.fori_loop(0, rows // ROW, band, None)


BLOCKS = 4


def _update_some(attn_steps, arrays, table_ref, *refs):
    heads = PAIR // HEAD
    g_refs, refs = refs[: SLOTS * arrays], refs[SLOTS * arrays :]
    step = pl.program_id(0) - attn_steps
    if attn_steps:
        units, refs = refs[:heads], refs[heads:]
        old, new, mlp_old, mlp_new = refs[:12], refs[21:33], refs[12:21], refs[33:]

        @pl.when(step < 0)
        def _():
            for n in range(4):
                wide, rows = (1, 512) if n < 3 else (SIDE, HEAD)
                view = lambda x, j: x.at[:, pl.ds(j * HEAD, HEAD)] if n < 3 else x.at[pl.ds(j * HEAD, HEAD)]
                olds, news = ([[view(x, j) for x in xs[3 * n : 3 * n + 3]] for j in range(heads)] for xs in (old, new))
                _update(lambda b, r, c: units[b][0, 0, CHUNKS[0] * n + r * wide + c], olds, news, wide, rows)

    else:
        mlp_old, mlp_new = refs[:9], refs[-9:]

    def views(three, tall):
        return [[(x.at[b, 0] if tall else x.at[0, :, pl.ds(b * FT, FT)]) for x in three] for b in range(BLOCKS)]

    for n in range(arrays):

        @pl.when((step >= BLOCKS * n) & (step < BLOCKS * (n + 1)))
        def _(n=n):
            for c in range(SLOTS):
                olds, news = (views(x[3 * c : 3 * c + 3], c == 2) for x in (mlp_old, mlp_new))
                _update(lambda b, r, k: g_refs[SLOTS * n + c][b, r * SIDE + k], olds, news, SIDE, LANE)


def update_some(table, arrays, old, so_far=(), attn=None, attn_old=()):
    heads = PAIR // HEAD
    views, spots = [], []
    attn_steps = attn_old[0].shape[1] // PAIR if attn_old else 0
    at = lambda s: jnp.maximum(s - attn_steps, 0)
    for c, w in enumerate(old[::3]):
        rows, columns = w.shape
        if c == 2:
            views.append((rows // FT, SIDE, LANE, columns))
            spots.append(pl.BlockSpec((BLOCKS, 1, LANE, columns), lambda s, t, c=c: (_rem(at(s), BLOCKS), t[c, lax.div(at(s), BLOCKS)], 0, 0)))
        else:
            views.append((SIDE, LANE, columns))
            spots.append(pl.BlockSpec((1, LANE, BLOCKS * FT), lambda s, t, c=c: (t[c, lax.div(at(s), BLOCKS)], 0, _rem(at(s), BLOCKS))))
    g_specs = [pl.BlockSpec((BLOCKS, *g.shape[1:]), lambda s, t, n=n: (jnp.clip(at(s) - BLOCKS * n, 0, BLOCKS - 1), 0, 0, 0))
               for n, g in zip([k // SLOTS for k in range(len(arrays))], arrays)]
    all_views, all_spots = ([x for x in xs for _ in range(3)] for xs in (views, spots))
    given = [x.reshape(view) for x, view in zip(old, all_views)]
    extra, extra_specs, attn_specs = [], [], []
    if attn_steps:
        first = lambda s: jnp.minimum(s, attn_steps - 1)
        extra = [attn] * heads
        for j in range(heads):
            head = lambda s, j=j: heads * first(s) + j
            extra_specs.append(pl.BlockSpec((1, 1, *attn.shape[2:]), lambda s, t, head=head: (lax.div(head(s), SLOTS), _rem(head(s), SLOTS), 0, 0, 0)))
        d = attn_old[0].shape[0]
        attn_specs = [pl.BlockSpec((d, PAIR), lambda s, t: (0, first(s)))] * 9 + [pl.BlockSpec((PAIR, d), lambda s, t: (first(s), 0))] * 3
    operands = [*arrays, *extra, *attn_old, *given, *so_far]
    results = [*attn_old, *given]
    return pl.pallas_call(
        functools.partial(_update_some, attn_steps, len(arrays) // SLOTS),
        grid_spec=pltpu.PrefetchScalarGridSpec(
            num_scalar_prefetch=1,
            grid=(attn_steps + BLOCKS * len(arrays) // SLOTS,),
            in_specs=g_specs + extra_specs + attn_specs + all_spots + [pl.BlockSpec(memory_space=pl.ANY)] * len(so_far),
            out_specs=attn_specs + all_spots,
        ),
        out_shape=[jax.ShapeDtypeStruct(x.shape, x.dtype) for x in results],
        input_output_aliases={1 + len(operands) - len(so_far) + n: n for n in range(len(so_far))},
        compiler_params=pltpu.CompilerParams(dimension_semantics=("arbitrary",), vmem_limit_bytes=VMEM),
        cost_estimate=pl.CostEstimate(flops=sum(g.size for g in arrays) * 16, transcendentals=0, bytes_accessed=sum(g.size for g in arrays) * 22),
        name="update",
    )(table, *operands)


def shifted(axis, by):
    stride = SIDE ** (2 - axis)
    return [(d, d + ((d // stride % SIDE + by) % SIDE - d // stride % SIDE) * stride) for d in range(SIDE**3)]


def solution(mesh):
    def step(x, dy, *arrays):
        weights, m, v = ([a[0] for a in arrays[i : i + 7]] for i in (0, 7, 14))
        old = [a for three in zip(weights, m, v) for a in three]
        h = x[0]
        wq, wk, wv, wo, wg, wu, wd = weights
        cos, sin = angles(h.shape[0])
        q, k, v_, ot, lse, h1 = attn_fwd(h, cos, sin, wq, wk, wv, wo)
        *own, attn = backward(h, h1, dy[0], wg, wu, wd, cos, sin, q, k, v_, ot, lse, wo)
        move = lambda arrays, by: [lax.ppermute(a, "dp", shifted(n, by)) for n, a in enumerate(arrays)]
        back, ahead = move(own, 1), move(own, -1)
        far = move(back, 1)
        places = jnp.stack([places[0] for places, _ in _spots()])
        table = lambda *away: (places[:, None] + jnp.array(away, jnp.int32)) % SIDE
        new = update_some(table(0), own, old[12:], (), attn, old[:12])
        new_attn, new = [*new[:12]], new[12:]
        new = update_some(table(3, 1), back + ahead, old[12:], new)
        new = update_some(table(2), far, old[12:], new)
        new = new_attn + [a.reshape(b.shape) for a, b in zip(new, old[12:])]
        return tuple(a[None] for which in range(3) for a in new[which::3])

    states, all_of = P(("rep", "dp"), None, None), P(None, None, None)
    return jax.shard_map(
        step,
        mesh=mesh,
        in_specs=(states, states) + (all_of,) * 21,
        out_specs=(P("rep", None, None),) * 21,
        check_vma=False,
    )
```
